32 devices in a mesh: band: 4 (over y, x), ga: 8 (over z, core).
Axes of the slice: x: 2, y: 2, z: 4, core: 2. Of those that a mesh axis runs over, the one named last changes fastest.
Arguments:
- orbitals: bfloat16 [8192, 1024], P('ga', 'band'), may hold values from -6 to 6
Outputs:
- margin: float32 [1024, 1024], P('band', 'ga')
- corrected: bfloat16 [8192, 1024], P('ga', 'band')
The draws below stay inside these ranges and needn't reach their ends.
All inputs are finite; a program needn't handle non-finite values.
Results may differ from the reference program's by a relative error of at most 0.0056.
Values may be sent and summed in bfloat16 or wider, within the bound.
No kernel may reach another device: no remote copies, remote signals or barrier semaphores. Data moves between devices by JAX's collectives and lax.ppermute only.
A program may use at most 64 MiB of HBM per device.

```python
import jax
import jax.numpy as jnp
from jax import lax

NB = 1024
NG = 8192


def draw_orbitals(key, part):
    first = jax.random.fold_in(key, 0)
    values = jnp.clip(jax.random.normal(first, (NG, NB), jnp.float32), -6.0, 6.0)
    return values.astype(jnp.bfloat16)


def setup_inputs(seed: int = 0) -> dict:
    streams_of = jax.random.split(jax.random.key(seed), 2)
    orbitals = draw_orbitals(jax.random.fold_in(streams_of[1], 71), 0)
    return dict(orbitals=orbitals)


def reference(orbitals):
    margin = jnp.dot(orbitals.T, orbitals, preferred_element_type=jnp.float32) / NG
    identity = jnp.eye(NB, dtype=jnp.float32)
    deviation = margin - identity
    square = jnp.dot(deviation, deviation, precision=lax.Precision.HIGHEST, preferred_element_type=jnp.float32)
    correction = (identity - 0.5 * deviation + 0.375 * square).astype(jnp.bfloat16)
    corrected = jnp.dot(orbitals, correction, preferred_element_type=jnp.float32).astype(jnp.bfloat16)
    return (margin, corrected)
```

```python
import functools

import jax
import jax.numpy as jnp
from jax import lax
from jax.experimental import pallas as pl
from jax.experimental.pallas import tpu as pltpu
from jax.sharding import PartitionSpec as P

VMEM = pl.BlockSpec(memory_space=pltpu.VMEM)


def swap(value, axis, mask):
    size = lax.axis_size(axis)
    return lax.ppermute(value, axis, [(i, i ^ mask) for i in range(size)])


def gather_bands(orbitals):
    size = lax.axis_size("band")
    half = orbitals.shape[0] // 2
    pieces = [orbitals[:half], orbitals[half:]]
    if size != 4:
        everyone = lax.all_gather(orbitals, "band", axis=0)
        me = lax.axis_index("band")
        others = [
            lax.dynamic_index_in_dim(everyone, me ^ r, keepdims=False) for r in range(1, size)
        ]
        return [pieces] + [[o[:half], o[half:]] for o in others]
    top, low = pieces
    top1, low2 = swap(top, "band", 1), swap(low, "band", 2)
    low1, top2 = swap(low, "band", 1), swap(top, "band", 2)
    top3, low3 = swap(top1, "band", 2), swap(low2, "band", 1)
    return [pieces, [top1, low1], [top2, low2], [top3, low3]]


def partial_kernel(groups, chips, own_ref, *refs):
    parts, (keep_ref, send_ref) = refs[:-2], refs[-2:]
    band, ga = lax.axis_index("band"), lax.axis_index("ga")
    is_first = lax.rem(ga, 2) == 0
    chip = ga // 2
    pairs = chips // groups
    width = keep_ref.shape[2]
    half = own_ref.shape[0] // 2
    for r in range(groups):
        if r == 0:
            block = lax.dot_general(
                own_ref[...], own_ref[...], (((0,), (0,)), ((), ())),
                preferred_element_type=jnp.float32,
            )
        else:
            top, low = parts[2 * r - 2], parts[2 * r - 1]
            block = lax.dot_general(
                own_ref[:half, :], top[...], (((0,), (0,)), ((), ())),
                preferred_element_type=jnp.float32,
            ) + lax.dot_general(
                own_ref[half:, :], low[...], (((0,), (0,)), ((), ())),
                preferred_element_type=jnp.float32,
            )
        for j in range(pairs):
            place = ((band ^ r) * pairs + j) ^ chip
            left = block[:, 2 * j * width : (2 * j + 1) * width]
            right = block[:, (2 * j + 1) * width : (2 * j + 2) * width]
            keep_ref[place] = jnp.where(is_first, left, right)
            send_ref[place] = jnp.where(is_first, right, left).astype(send_ref.dtype)


def fix_kernel(groups, chips, margin_ref, own_ref, *refs):
    rows, other_ref = refs[: chips - 1], refs[chips - 1]
    cols = refs[chips : chips + groups - 1]
    fix_ref, cols_ref = refs[-2:]
    band, ga = lax.axis_index("band"), lax.axis_index("ga")
    chip, core = ga // 2, lax.rem(ga, 2)
    height, width = margin_ref.shape
    for r in range(groups):
        source = own_ref if r == 0 else cols[r - 1]
        cols_ref[pl.ds(pl.multiple_of((band ^ r) * height, height), height), :] = source[...]
    square = jnp.zeros((height, width), jnp.float32)
    for i in range(chips):
        place = (chip ^ i) * 2
        mine = own_ref if i == 0 else rows[i - 1]
        for block, owner in ((mine[...], place + core), (other_ref[i], place + 1 - core)):
            depth = pl.ds(pl.multiple_of(owner * width, width), width)
            square += jnp.dot(block, cols_ref[depth, :], preferred_element_type=jnp.float32)
    row_index = band * height + lax.broadcasted_iota(jnp.int32, (height, width), 0)
    col_index = ga * width + lax.broadcasted_iota(jnp.int32, (height, width), 1)
    unit = (row_index == col_index).astype(jnp.float32)
    deviation = margin_ref[...] - unit
    fix_ref[...] = (unit - 0.5 * deviation + 0.375 * square).astype(fix_ref.dtype)


def final_kernel(groups, chips, orbitals_ref, *refs):
    parts = refs[: 2 * (groups - 1)]
    fix_own = refs[2 * (groups - 1)]
    fix_rows = refs[2 * groups - 1 : 2 * groups - 2 + chips]
    other_ref = refs[2 * groups - 2 + chips]
    out_ref, fix_ref = refs[-2:]
    band, ga = lax.axis_index("band"), lax.axis_index("ga")
    chip, core = ga // 2, lax.rem(ga, 2)
    width = fix_own.shape[1]
    for i in range(chips):
        mine = fix_own if i == 0 else fix_rows[i - 1]
        place = (chip ^ i) * 2
        fix_ref[place + core] = mine[...]
        fix_ref[place + 1 - core] = other_ref[i]
    half = orbitals_ref.shape[0] // 2
    share = 2 * chips // groups
    fixes = [
        jnp.concatenate([fix_ref[(band ^ r) * share + j] for j in range(share)], axis=1)
        for r in range(groups)
    ]
    for s in range(2):
        total = None
        for r in range(groups):
            if r == 0:
                piece = orbitals_ref[s * half : (s + 1) * half, :]
            else:
                piece = parts[2 * r - 2 + s][...]
            term = lax.dot_general(
                piece, fixes[r], (((1,), (1,)), ((), ())), preferred_element_type=jnp.float32
            )
            total = term if total is None else total + term
        out_ref[s * half : (s + 1) * half, :] = total.astype(out_ref.dtype)


def call(kernel, outs, *args, scratch=(), flops=0):
    return pl.pallas_call(
        kernel,
        out_shape=outs,
        in_specs=[VMEM] * len(args),
        out_specs=jax.tree.map(lambda _: VMEM, outs),
        scratch_shapes=list(scratch),
        cost_estimate=pl.CostEstimate(flops=flops, bytes_accessed=0, transcendentals=0),
    )(*args)


def gather_chips(block, chips):
    rows = [swap(block, "ga", 2 * i) for i in range(1, chips)]
    other = swap(jnp.stack([block] + rows), "ga", 1)
    return rows, other


def shards(orbitals):
    own_coeffs, own_bands = orbitals.shape
    groups, size = lax.axis_size("band"), lax.axis_size("ga")
    chips = size // 2
    all_bands = own_bands * groups
    all_coeffs = own_coeffs * size
    width = all_bands // size
    row_start = lax.axis_index("band") * own_bands
    col_start = lax.axis_index("ga") * width

    bands = gather_bands(orbitals)
    parts = [piece for pieces in bands[1:] for piece in pieces]
    keep, send = call(
        functools.partial(partial_kernel, groups, chips),
        (
            jax.ShapeDtypeStruct((chips, own_bands, width), jnp.float32),
            jax.ShapeDtypeStruct((chips, own_bands, width), jnp.bfloat16),
        ),
        orbitals,
        *parts,
        flops=2 * own_coeffs * own_bands * all_bands,
    )
    chip_sum = keep + swap(send, "ga", 1).astype(jnp.float32)
    total = chip_sum[0]
    for i in range(1, chips):
        total += swap(chip_sum[i].astype(jnp.bfloat16), "ga", 2 * i).astype(jnp.float32)
    margin_block = total / all_coeffs

    row_index = row_start + lax.iota(jnp.int32, own_bands)
    col_index = col_start + lax.iota(jnp.int32, width)
    unit_block = (row_index[:, None] == col_index[None, :]).astype(jnp.float32)
    deviation = (margin_block - unit_block).astype(jnp.bfloat16)
    rows, other = gather_chips(deviation, chips)
    cols = [swap(deviation, "band", r) for r in range(1, groups)]
    fix_block = call(
        functools.partial(fix_kernel, groups, chips),
        jax.ShapeDtypeStruct((own_bands, width), jnp.bfloat16),
        margin_block,
        deviation,
        *rows,
        other,
        *cols,
        scratch=[pltpu.VMEM((all_bands, width), jnp.bfloat16)],
        flops=2 * own_bands * all_bands * width,
    )
    fix_rows, fix_other = gather_chips(fix_block, chips)
    corrected = call(
        functools.partial(final_kernel, groups, chips),
        jax.ShapeDtypeStruct(orbitals.shape, jnp.bfloat16),
        orbitals,
        *parts,
        fix_block,
        *fix_rows,
        fix_other,
        scratch=[pltpu.VMEM((size, own_bands, width), jnp.bfloat16)],
        flops=2 * own_coeffs * own_bands * all_bands,
    )
    return (margin_block, corrected)


def solution(mesh):
    return jax.shard_map(
        shards,
        mesh=mesh,
        in_specs=(P("ga", "band"),),
        out_specs=(P("band", "ga"), P("ga", "band")),
        check_vma=False,
    )
```

```python
import functools

import jax
import jax.numpy as jnp
from jax import lax
from jax.experimental import pallas as pl
from jax.experimental.pallas import tpu as pltpu
from jax.sharding import PartitionSpec as P

GRANT = 4 * 2**20
VMEM = pl.BlockSpec(memory_space=pltpu.VMEM)


def swap(value, axis, mask):
    size = lax.axis_size(axis)
    return lax.ppermute(value, axis, [(i, i ^ mask) for i in range(size)])


def gather_bands(orbitals):
    size = lax.axis_size("band")
    half = orbitals.shape[0] // 2
    pieces = [orbitals[:half], orbitals[half:]]
    if size != 4:
        everyone = lax.all_gather(orbitals, "band", axis=0)
        me = lax.axis_index("band")
        others = [
            lax.dynamic_index_in_dim(everyone, me ^ r, keepdims=False) for r in range(1, size)
        ]
        return [pieces] + [[o[:half], o[half:]] for o in others]
    top, low = pieces
    top1, low2 = swap(top, "band", 1), swap(low, "band", 2)
    low1, top2 = swap(low, "band", 1), swap(top, "band", 2)
    top3, low3 = swap(top1, "band", 2), swap(low2, "band", 1)
    return [pieces, [top1, low1], [top2, low2], [top3, low3]]


def partial_kernel(groups, chips, own_ref, *refs):
    parts, (keep_ref, send_ref) = refs[:-2], refs[-2:]
    band, ga = lax.axis_index("band"), lax.axis_index("ga")
    is_first = lax.rem(ga, 2) == 0
    chip = ga // 2
    pairs = chips // groups
    width = keep_ref.shape[2]
    half = own_ref.shape[0] // 2
    for r in range(groups):
        if r == 0:
            block = lax.dot_general(
                own_ref[...], own_ref[...], (((0,), (0,)), ((), ())),
                preferred_element_type=jnp.float32,
            )
        else:
            top, low = parts[2 * r - 2], parts[2 * r - 1]
            block = lax.dot_general(
                own_ref[:half, :], top[...], (((0,), (0,)), ((), ())),
                preferred_element_type=jnp.float32,
            ) + lax.dot_general(
                own_ref[half:, :], low[...], (((0,), (0,)), ((), ())),
                preferred_element_type=jnp.float32,
            )
        for j in range(pairs):
            place = ((band ^ r) * pairs + j) ^ chip
            left = block[:, 2 * j * width : (2 * j + 1) * width]
            right = block[:, (2 * j + 1) * width : (2 * j + 2) * width]
            keep_ref[place] = jnp.where(is_first, left, right)
            send_ref[place] = jnp.where(is_first, right, left).astype(send_ref.dtype)


def fix_kernel(groups, chips, margin_ref, own_ref, *refs):
    rows, other_ref = refs[: chips - 1], refs[chips - 1]
    cols = refs[chips : chips + groups - 1]
    fix_ref, cols_ref = refs[-2:]
    band, ga = lax.axis_index("band"), lax.axis_index("ga")
    chip, core = ga // 2, lax.rem(ga, 2)
    height, width = margin_ref.shape
    for r in range(groups):
        source = own_ref if r == 0 else cols[r - 1]
        cols_ref[pl.ds(pl.multiple_of((band ^ r) * height, height), height), :] = source[...]
    square = jnp.zeros((height, width), jnp.float32)
    for i in range(chips):
        place = (chip ^ i) * 2
        mine = own_ref if i == 0 else rows[i - 1]
        for block, owner in ((mine[...], place + core), (other_ref[i], place + 1 - core)):
            depth = pl.ds(pl.multiple_of(owner * width, width), width)
            square += jnp.dot(block, cols_ref[depth, :], preferred_element_type=jnp.float32)
    row_index = band * height + lax.broadcasted_iota(jnp.int32, (height, width), 0)
    col_index = ga * width + lax.broadcasted_iota(jnp.int32, (height, width), 1)
    unit = (row_index == col_index).astype(jnp.float32)
    deviation = margin_ref[...] - unit
    fix_ref[...] = (unit - 0.5 * deviation + 0.375 * square).astype(fix_ref.dtype)


def final_kernel(groups, chips, orbitals_ref, *refs):
    parts = refs[: 2 * (groups - 1)]
    fix_own = refs[2 * (groups - 1)]
    fix_rows = refs[2 * groups - 1 : 2 * groups - 2 + chips]
    other_ref = refs[2 * groups - 2 + chips]
    out_ref, fix_ref = refs[-2:]
    band, ga = lax.axis_index("band"), lax.axis_index("ga")
    chip, core = ga // 2, lax.rem(ga, 2)
    width = fix_own.shape[1]
    for i in range(chips):
        mine = fix_own if i == 0 else fix_rows[i - 1]
        place = (chip ^ i) * 2
        fix_ref[place + core] = mine[...]
        fix_ref[place + 1 - core] = other_ref[i]
    half = orbitals_ref.shape[0] // 2
    share = 2 * chips // groups
    fixes = [
        jnp.concatenate([fix_ref[(band ^ r) * share + j] for j in range(share)], axis=1)
        for r in range(groups)
    ]
    for s in range(2):
        total = None
        for r in range(groups):
            if r == 0:
                piece = orbitals_ref[s * half : (s + 1) * half, :]
            else:
                piece = parts[2 * r - 2 + s][...]
            term = lax.dot_general(
                piece, fixes[r], (((1,), (1,)), ((), ())), preferred_element_type=jnp.float32
            )
            total = term if total is None else total + term
        out_ref[s * half : (s + 1) * half, :] = total.astype(out_ref.dtype)


def size_of(value):
    return value.size * value.dtype.itemsize


def call(kernel, outs, *args, scratch=(), flops=0):
    held = sum(size_of(leaf) for leaf in [*args, *jax.tree.leaves(outs)])
    return pl.pallas_call(
        kernel,
        out_shape=outs,
        in_specs=[VMEM] * len(args),
        out_specs=jax.tree.map(lambda _: VMEM, outs),
        scratch_shapes=list(scratch),
        cost_estimate=pl.CostEstimate(flops=flops, bytes_accessed=0, transcendentals=0),
        compiler_params=pltpu.CompilerParams(vmem_limit_bytes=min(2 * held + GRANT, 60 * GRANT // 4)),
    )(*args)


def gather_chips(block, chips):
    rows = [swap(block, "ga", 2 * i) for i in range(1, chips)]
    other = swap(jnp.stack([block] + rows), "ga", 1)
    return rows, other


def shards(orbitals):
    own_coeffs, own_bands = orbitals.shape
    groups, size = lax.axis_size("band"), lax.axis_size("ga")
    chips = size // 2
    all_bands = own_bands * groups
    all_coeffs = own_coeffs * size
    width = all_bands // size
    row_start = lax.axis_index("band") * own_bands
    col_start = lax.axis_index("ga") * width

    bands = gather_bands(orbitals)
    parts = [piece for pieces in bands[1:] for piece in pieces]
    keep, send = call(
        functools.partial(partial_kernel, groups, chips),
        (
            jax.ShapeDtypeStruct((chips, own_bands, width), jnp.float32),
            jax.ShapeDtypeStruct((chips, own_bands, width), jnp.bfloat16),
        ),
        orbitals,
        *parts,
        flops=2 * own_coeffs * own_bands * all_bands,
    )
    chip_sum = keep + swap(send, "ga", 1).astype(jnp.float32)
    total = chip_sum[0]
    for i in range(1, chips):
        total += swap(chip_sum[i].astype(jnp.bfloat16), "ga", 2 * i).astype(jnp.float32)
    margin_block = total / all_coeffs

    row_index = row_start + lax.iota(jnp.int32, own_bands)
    col_index = col_start + lax.iota(jnp.int32, width)
    unit_block = (row_index[:, None] == col_index[None, :]).astype(jnp.float32)
    deviation = (margin_block - unit_block).astype(jnp.bfloat16)
    rows, other = gather_chips(deviation, chips)
    cols = [swap(deviation, "band", r) for r in range(1, groups)]
    fix_block = call(
        functools.partial(fix_kernel, groups, chips),
        jax.ShapeDtypeStruct((own_bands, width), jnp.bfloat16),
        margin_block,
        deviation,
        *rows,
        other,
        *cols,
        scratch=[pltpu.VMEM((all_bands, width), jnp.bfloat16)],
        flops=2 * own_bands * all_bands * width,
    )
    fix_rows, fix_other = gather_chips(fix_block, chips)
    corrected = call(
        functools.partial(final_kernel, groups, chips),
        jax.ShapeDtypeStruct(orbitals.shape, jnp.bfloat16),
        orbitals,
        *parts,
        fix_block,
        *fix_rows,
        fix_other,
        scratch=[pltpu.VMEM((size, own_bands, width), jnp.bfloat16)],
        flops=2 * own_coeffs * own_bands * all_bands,
    )
    return (margin_block, corrected)


def solution(mesh):
    return jax.shard_map(
        shards,
        mesh=mesh,
        in_specs=(P("ga", "band"),),
        out_specs=(P("band", "ga"), P("ga", "band")),
        check_vma=False,
    )
```

```python
import functools

import jax
import jax.numpy as jnp
from jax import lax
from jax.experimental import pallas as pl
from jax.experimental.pallas import tpu as pltpu
from jax.sharding import PartitionSpec as P

GRANT = 4 * 2**20
VMEM = pl.BlockSpec(memory_space=pltpu.VMEM)


def swap(value, axis, mask):
    size = lax.axis_size(axis)
    return lax.ppermute(value, axis, [(i, i ^ mask) for i in range(size)])


def gather_bands(orbitals):
    size = lax.axis_size("band")
    half = orbitals.shape[0] // 2
    pieces = [orbitals[:half], orbitals[half:]]
    if size != 4:
        everyone = lax.all_gather(orbitals, "band", axis=0)
        me = lax.axis_index("band")
        others = [
            lax.dynamic_index_in_dim(everyone, me ^ r, keepdims=False) for r in range(1, size)
        ]
        return [pieces] + [[o[:half], o[half:]] for o in others]
    top, low = pieces
    top1, low2 = swap(top, "band", 1), swap(low, "band", 2)
    low1, top2 = swap(low, "band", 1), swap(top, "band", 2)
    top3, low3 = swap(top1, "band", 2), swap(low2, "band", 1)
    return [pieces, [top1, low1], [top2, low2], [top3, low3]]


def partial_kernel(groups, chips, own_ref, *refs):
    parts, (keep_ref, send_ref) = refs[:-2], refs[-2:]
    band, ga = lax.axis_index("band"), lax.axis_index("ga")
    is_first = lax.rem(ga, 2) == 0
    chip = ga // 2
    pairs = chips // groups
    width = keep_ref.shape[2]
    half = own_ref.shape[0] // 2
    for r in range(groups):
        if r == 0:
            block = lax.dot_general(
                own_ref[...], own_ref[...], (((0,), (0,)), ((), ())),
                preferred_element_type=jnp.float32,
            )
        else:
            top, low = parts[2 * r - 2], parts[2 * r - 1]
            block = lax.dot_general(
                own_ref[:half, :], top[...], (((0,), (0,)), ((), ())),
                preferred_element_type=jnp.float32,
            ) + lax.dot_general(
                own_ref[half:, :], low[...], (((0,), (0,)), ((), ())),
                preferred_element_type=jnp.float32,
            )
        for j in range(pairs):
            place = ((band ^ r) * pairs + j) ^ chip
            left = block[:, 2 * j * width : (2 * j + 1) * width]
            right = block[:, (2 * j + 1) * width : (2 * j + 2) * width]
            keep_ref[place] = jnp.where(is_first, left, right)
            send_ref[place] = jnp.where(is_first, right, left).astype(send_ref.dtype)


def fix_kernel(groups, chips, margin_ref, own_ref, *refs):
    rows, other_ref = refs[: chips - 1], refs[chips - 1]
    cols = refs[chips : chips + groups - 1]
    fix_ref, cols_ref = refs[-2:]
    band, ga = lax.axis_index("band"), lax.axis_index("ga")
    chip, core = ga // 2, lax.rem(ga, 2)
    height, width = margin_ref.shape
    for r in range(groups):
        source = own_ref if r == 0 else cols[r - 1]
        cols_ref[pl.ds(pl.multiple_of((band ^ r) * height, height), height), :] = source[...]
    square = jnp.zeros((height, width), jnp.float32)
    for i in range(chips):
        place = (chip ^ i) * 2
        mine = own_ref if i == 0 else rows[i - 1]
        for block, owner in ((mine[...], place + core), (other_ref[i], place + 1 - core)):
            depth = pl.ds(pl.multiple_of(owner * width, width), width)
            square += jnp.dot(block, cols_ref[depth, :], preferred_element_type=jnp.float32)
    row_index = band * height + lax.broadcasted_iota(jnp.int32, (height, width), 0)
    col_index = ga * width + lax.broadcasted_iota(jnp.int32, (height, width), 1)
    unit = (row_index == col_index).astype(jnp.float32)
    deviation = margin_ref[...] - unit
    fix_ref[...] = (unit - 0.5 * deviation + 0.375 * square).astype(fix_ref.dtype)


def final_kernel(groups, chips, orbitals_ref, *refs):
    parts = refs[: 2 * (groups - 1)]
    fix_own = refs[2 * (groups - 1)]
    fix_rows = refs[2 * groups - 1 : 2 * groups - 2 + chips]
    other_ref = refs[2 * groups - 2 + chips]
    out_ref, fix_ref = refs[-2:]
    band, ga = lax.axis_index("band"), lax.axis_index("ga")
    chip, core = ga // 2, lax.rem(ga, 2)
    width = fix_own.shape[1]
    for i in range(chips):
        mine = fix_own if i == 0 else fix_rows[i - 1]
        place = (chip ^ i) * 2
        fix_ref[place + core] = mine[...]
        fix_ref[place + 1 - core] = other_ref[i]
    half = orbitals_ref.shape[0] // 2
    share = 2 * chips // groups
    fixes = [
        jnp.concatenate([fix_ref[(band ^ r) * share + j] for j in range(share)], axis=1)
        for r in range(groups)
    ]
    for s in range(2):
        total = None
        for r in range(groups):
            if r == 0:
                piece = orbitals_ref[s * half : (s + 1) * half, :]
            else:
                piece = parts[2 * r - 2 + s][...]
            term = lax.dot_general(
                piece, fixes[r], (((1,), (1,)), ((), ())), preferred_element_type=jnp.float32
            )
            total = term if total is None else total + term
        out_ref[s * half : (s + 1) * half, :] = total.astype(out_ref.dtype)


def size_of(value):
    return value.size * value.dtype.itemsize


def call(kernel, outs, *args, scratch=(), flops=0):
    held = sum(size_of(leaf) for leaf in [*args, *jax.tree.leaves(outs)])
    return pl.pallas_call(
        kernel,
        out_shape=outs,
        in_specs=[VMEM] * len(args),
        out_specs=jax.tree.map(lambda _: VMEM, outs),
        scratch_shapes=list(scratch),
        cost_estimate=pl.CostEstimate(flops=flops, bytes_accessed=0, transcendentals=0),
        compiler_params=pltpu.CompilerParams(vmem_limit_bytes=min(2 * held + GRANT, 60 * GRANT // 4)),
    )(*args)


def gather_chips(block, chips, beside=0):
    rows = [swap(block, "ga", 2 * i) for i in range(1, chips)]
    cols = [swap(block, "band", r) for r in range(1, beside + 1)]
    rows, cols = lax.optimization_barrier((rows, cols))
    other = swap(jnp.stack([block] + rows), "ga", 1)
    return rows, other, cols


def shards(orbitals):
    own_coeffs, own_bands = orbitals.shape
    groups, size = lax.axis_size("band"), lax.axis_size("ga")
    chips = size // 2
    all_bands = own_bands * groups
    all_coeffs = own_coeffs * size
    width = all_bands // size
    row_start = lax.axis_index("band") * own_bands
    col_start = lax.axis_index("ga") * width

    bands = gather_bands(orbitals)
    parts = [piece for pieces in bands[1:] for piece in pieces]
    keep, send = call(
        functools.partial(partial_kernel, groups, chips),
        (
            jax.ShapeDtypeStruct((chips, own_bands, width), jnp.float32),
            jax.ShapeDtypeStruct((chips, own_bands, width), jnp.bfloat16),
        ),
        orbitals,
        *parts,
        flops=2 * own_coeffs * own_bands * all_bands,
    )
    chip_sum = keep + swap(send, "ga", 1).astype(jnp.float32)
    total = chip_sum[0]
    for i in range(1, chips):
        total += swap(chip_sum[i].astype(jnp.bfloat16), "ga", 2 * i).astype(jnp.float32)
    margin_block = total / all_coeffs

    row_index = row_start + lax.iota(jnp.int32, own_bands)
    col_index = col_start + lax.iota(jnp.int32, width)
    unit_block = (row_index[:, None] == col_index[None, :]).astype(jnp.float32)
    deviation = (margin_block - unit_block).astype(jnp.bfloat16)
    rows, other, cols = gather_chips(deviation, chips, groups - 1)
    fix_block = call(
        functools.partial(fix_kernel, groups, chips),
        jax.ShapeDtypeStruct((own_bands, width), jnp.bfloat16),
        margin_block,
        deviation,
        *rows,
        other,
        *cols,
        scratch=[pltpu.VMEM((all_bands, width), jnp.bfloat16)],
        flops=2 * own_bands * all_bands * width,
    )
    fix_rows, fix_other, _ = gather_chips(fix_block, chips)
    corrected = call(
        functools.partial(final_kernel, groups, chips),
        jax.ShapeDtypeStruct(orbitals.shape, jnp.bfloat16),
        orbitals,
        *parts,
        fix_block,
        *fix_rows,
        fix_other,
        scratch=[pltpu.VMEM((size, own_bands, width), jnp.bfloat16)],
        flops=2 * own_coeffs * own_bands * all_bands,
    )
    return (margin_block, corrected)


def solution(mesh):
    return jax.shard_map(
        shards,
        mesh=mesh,
        in_specs=(P("ga", "band"),),
        out_specs=(P("band", "ga"), P("ga", "band")),
        check_vma=False,
    )
```

```python
import functools

import jax
import jax.numpy as jnp
from jax import lax
from jax.experimental import pallas as pl
from jax.experimental.pallas import tpu as pltpu
from jax.sharding import PartitionSpec as P

GRANT = 4 * 2**20
VMEM = pl.BlockSpec(memory_space=pltpu.VMEM)


def swap(value, axis, mask):
    size = lax.axis_size(axis)
    return lax.ppermute(value, axis, [(i, i ^ mask) for i in range(size)])


def gather_bands(orbitals):
    size = lax.axis_size("band")
    half = orbitals.shape[0] // 2
    pieces = [orbitals[:half], orbitals[half:]]
    if size != 4:
        everyone = lax.all_gather(orbitals, "band", axis=0)
        me = lax.axis_index("band")
        others = [
            lax.dynamic_index_in_dim(everyone, me ^ r, keepdims=False) for r in range(1, size)
        ]
        return [pieces] + [[o[:half], o[half:]] for o in others]
    top, low = pieces
    top1, low2 = swap(top, "band", 1), swap(low, "band", 2)
    low1, top2 = swap(low, "band", 1), swap(top, "band", 2)
    top3, low3 = swap(top1, "band", 2), swap(low2, "band", 1)
    return [pieces, [top1, low1], [top2, low2], [top3, low3]]


def partial_kernel(groups, chips, own_ref, *refs):
    parts, (keep_ref, send_ref) = refs[:-2], refs[-2:]
    band, ga = lax.axis_index("band"), lax.axis_index("ga")
    is_first = lax.rem(ga, 2) == 0
    chip = ga // 2
    pairs = chips // groups
    width = keep_ref.shape[2]
    half = own_ref.shape[0] // 2
    for r in range(groups):
        if r == 0:
            block = lax.dot_general(
                own_ref[...], own_ref[...], (((0,), (0,)), ((), ())),
                preferred_element_type=jnp.float32,
            )
        else:
            top, low = parts[2 * r - 2], parts[2 * r - 1]
            block = lax.dot_general(
                own_ref[:half, :], top[...], (((0,), (0,)), ((), ())),
                preferred_element_type=jnp.float32,
            ) + lax.dot_general(
                own_ref[half:, :], low[...], (((0,), (0,)), ((), ())),
                preferred_element_type=jnp.float32,
            )
        for j in range(pairs):
            place = ((band ^ r) * pairs + j) ^ chip
            left = block[:, 2 * j * width : (2 * j + 1) * width]
            right = block[:, (2 * j + 1) * width : (2 * j + 2) * width]
            keep_ref[place] = jnp.where(is_first, left, right)
            send_ref[place] = jnp.where(is_first, right, left).astype(send_ref.dtype)


def fix_kernel(groups, chips, margin_ref, own_ref, *refs):
    rows, other_ref = refs[: chips - 1], refs[chips - 1]
    cols = refs[chips : chips + groups - 1]
    fix_ref, cols_ref = refs[-2:]
    band, ga = lax.axis_index("band"), lax.axis_index("ga")
    chip, core = ga // 2, lax.rem(ga, 2)
    height, width = margin_ref.shape
    for r in range(groups):
        source = own_ref if r == 0 else cols[r - 1]
        cols_ref[pl.ds(pl.multiple_of((band ^ r) * height, height), height), :] = source[...]
    square = jnp.zeros((height, width), jnp.float32)
    for i in range(chips):
        place = (chip ^ i) * 2
        mine = own_ref if i == 0 else rows[i - 1]
        for block, owner in ((mine[...], place + core), (other_ref[i], place + 1 - core)):
            depth = pl.ds(pl.multiple_of(owner * width, width), width)
            square += jnp.dot(block, cols_ref[depth, :], preferred_element_type=jnp.float32)
    row_index = band * height + lax.broadcasted_iota(jnp.int32, (height, width), 0)
    col_index = ga * width + lax.broadcasted_iota(jnp.int32, (height, width), 1)
    unit = (row_index == col_index).astype(jnp.float32)
    deviation = margin_ref[...] - unit
    fix_ref[...] = (unit - 0.5 * deviation + 0.375 * square).astype(fix_ref.dtype)


def final_kernel(groups, chips, orbitals_ref, *refs):
    parts = refs[: 2 * (groups - 1)]
    fix_own = refs[2 * (groups - 1)]
    fix_rows = refs[2 * groups - 1 : 2 * groups - 2 + chips]
    other_ref = refs[2 * groups - 2 + chips]
    out_ref, fix_ref = refs[-2:]
    band, ga = lax.axis_index("band"), lax.axis_index("ga")
    chip, core = ga // 2, lax.rem(ga, 2)
    width = fix_own.shape[1]
    for i in range(chips):
        mine = fix_own if i == 0 else fix_rows[i - 1]
        place = (chip ^ i) * 2
        fix_ref[place + core] = mine[...]
        fix_ref[place + 1 - core] = other_ref[i]
    half = orbitals_ref.shape[0] // 2
    share = 2 * chips // groups
    fixes = [
        jnp.concatenate([fix_ref[(band ^ r) * share + j] for j in range(share)], axis=1)
        for r in range(groups)
    ]
    for s in range(2):
        total = None
        for r in range(groups):
            if r == 0:
                piece = orbitals_ref[s * half : (s + 1) * half, :]
            else:
                piece = parts[2 * r - 2 + s][...]
            term = lax.dot_general(
                piece, fixes[r], (((1,), (1,)), ((), ())), preferred_element_type=jnp.float32
            )
            total = term if total is None else total + term
        out_ref[s * half : (s + 1) * half, :] = total.astype(out_ref.dtype)


def size_of(value):
    return value.size * value.dtype.itemsize


def call(kernel, outs, *args, scratch=(), flops=0):
    held = sum(size_of(leaf) for leaf in [*args, *jax.tree.leaves(outs)])
    return pl.pallas_call(
        kernel,
        out_shape=outs,
        in_specs=[VMEM] * len(args),
        out_specs=jax.tree.map(lambda _: VMEM, outs),
        scratch_shapes=list(scratch),
        cost_estimate=pl.CostEstimate(flops=flops, bytes_accessed=0, transcendentals=0),
        compiler_params=pltpu.CompilerParams(vmem_limit_bytes=min(2 * held + GRANT, 60 * GRANT // 4)),
    )(*args)


def far_first(chips):
    return [*range(2, chips), *range(1, min(2, chips))]


def gather_chips(block, chips, beside=0):
    order = far_first(chips)
    moves = [("ga", 2 * i) for i in order[:-1]]
    moves += [("band", r) for r in range(beside, 0, -1)]
    moves += [("ga", 2 * i) for i in order[-1:]]
    landed = lax.optimization_barrier([swap(block, axis, mask) for axis, mask in moves])
    landed = dict(zip(moves, landed))
    rows = [landed["ga", 2 * i] for i in range(1, chips)]
    cols = [landed["band", r] for r in range(1, beside + 1)]
    other = swap(jnp.stack([block] + rows), "ga", 1)
    return rows, other, cols


def shards(orbitals):
    own_coeffs, own_bands = orbitals.shape
    groups, size = lax.axis_size("band"), lax.axis_size("ga")
    chips = size // 2
    all_bands = own_bands * groups
    all_coeffs = own_coeffs * size
    width = all_bands // size
    row_start = lax.axis_index("band") * own_bands
    col_start = lax.axis_index("ga") * width

    bands = gather_bands(orbitals)
    parts = [piece for pieces in bands[1:] for piece in pieces]
    keep, send = call(
        functools.partial(partial_kernel, groups, chips),
        (
            jax.ShapeDtypeStruct((chips, own_bands, width), jnp.float32),
            jax.ShapeDtypeStruct((chips, own_bands, width), jnp.bfloat16),
        ),
        orbitals,
        *parts,
        flops=2 * own_coeffs * own_bands * all_bands,
    )
    chip_sum = keep + swap(send, "ga", 1).astype(jnp.float32)
    total = chip_sum[0]
    for i in far_first(chips):
        total += swap(chip_sum[i].astype(jnp.bfloat16), "ga", 2 * i).astype(jnp.float32)
    margin_block = total / all_coeffs

    row_index = row_start + lax.iota(jnp.int32, own_bands)
    col_index = col_start + lax.iota(jnp.int32, width)
    unit_block = (row_index[:, None] == col_index[None, :]).astype(jnp.float32)
    deviation = (margin_block - unit_block).astype(jnp.bfloat16)
    rows, other, cols = gather_chips(deviation, chips, groups - 1)
    fix_block = call(
        functools.partial(fix_kernel, groups, chips),
        jax.ShapeDtypeStruct((own_bands, width), jnp.bfloat16),
        margin_block,
        deviation,
        *rows,
        other,
        *cols,
        scratch=[pltpu.VMEM((all_bands, width), jnp.bfloat16)],
        flops=2 * own_bands * all_bands * width,
    )
    fix_rows, fix_other, _ = gather_chips(fix_block, chips)
    corrected = call(
        functools.partial(final_kernel, groups, chips),
        jax.ShapeDtypeStruct(orbitals.shape, jnp.bfloat16),
        orbitals,
        *parts,
        fix_block,
        *fix_rows,
        fix_other,
        scratch=[pltpu.VMEM((size, own_bands, width), jnp.bfloat16)],
        flops=2 * own_coeffs * own_bands * all_bands,
    )
    return (margin_block, corrected)


def solution(mesh):
    return jax.shard_map(
        shards,
        mesh=mesh,
        in_specs=(P("ga", "band"),),
        out_specs=(P("band", "ga"), P("ga", "band")),
        check_vma=False,
    )
```

```python
import functools

import jax
import jax.numpy as jnp
from jax import lax
from jax.experimental import pallas as pl
from jax.experimental.pallas import tpu as pltpu
from jax.sharding import PartitionSpec as P

GRANT = 4 * 2**20
VMEM = pl.BlockSpec(memory_space=pltpu.VMEM)


def swap(value, axis, mask):
    size = lax.axis_size(axis)
    return lax.ppermute(value, axis, [(i, i ^ mask) for i in range(size)])


def gather_bands(orbitals):
    size = lax.axis_size("band")
    half = orbitals.shape[0] * 7 // 16
    pieces = [orbitals[:half], orbitals[half:]]
    if size != 4:
        everyone = lax.all_gather(orbitals, "band", axis=0)
        me = lax.axis_index("band")
        others = [
            lax.dynamic_index_in_dim(everyone, me ^ r, keepdims=False) for r in range(1, size)
        ]
        return [pieces] + [[o[:half], o[half:]] for o in others]
    top, low = pieces
    top1, low2 = swap(top, "band", 1), swap(low, "band", 2)
    low1, top2 = swap(low, "band", 1), swap(top, "band", 2)
    top3, low3 = swap(top1, "band", 2), swap(low2, "band", 1)
    return [pieces, [top1, low1], [top2, low2], [top3, low3]]


def partial_kernel(groups, chips, own_ref, *refs):
    parts, (keep_ref, send_ref) = refs[:-2], refs[-2:]
    band, ga = lax.axis_index("band"), lax.axis_index("ga")
    is_first = lax.rem(ga, 2) == 0
    chip = ga // 2
    pairs = chips // groups
    width = keep_ref.shape[2]
    half = parts[0].shape[0]
    for r in range(groups):
        if r == 0:
            block = lax.dot_general(
                own_ref[...], own_ref[...], (((0,), (0,)), ((), ())),
                preferred_element_type=jnp.float32,
            )
        else:
            top, low = parts[2 * r - 2], parts[2 * r - 1]
            block = lax.dot_general(
                own_ref[:half, :], top[...], (((0,), (0,)), ((), ())),
                preferred_element_type=jnp.float32,
            ) + lax.dot_general(
                own_ref[half:, :], low[...], (((0,), (0,)), ((), ())),
                preferred_element_type=jnp.float32,
            )
        for j in range(pairs):
            place = ((band ^ r) * pairs + j) ^ chip
            left = block[:, 2 * j * width : (2 * j + 1) * width]
            right = block[:, (2 * j + 1) * width : (2 * j + 2) * width]
            keep_ref[place] = jnp.where(is_first, left, right)
            send_ref[place] = jnp.where(is_first, right, left).astype(send_ref.dtype)


def fix_kernel(groups, chips, margin_ref, own_ref, *refs):
    rows, other_ref = refs[: chips - 1], refs[chips - 1]
    cols = refs[chips : chips + groups - 1]
    fix_ref, cols_ref = refs[-2:]
    band, ga = lax.axis_index("band"), lax.axis_index("ga")
    chip, core = ga // 2, lax.rem(ga, 2)
    height, width = margin_ref.shape
    for r in range(groups):
        source = own_ref if r == 0 else cols[r - 1]
        cols_ref[pl.ds(pl.multiple_of((band ^ r) * height, height), height), :] = source[...]
    square = jnp.zeros((height, width), jnp.float32)
    for i in range(chips):
        place = (chip ^ i) * 2
        mine = own_ref if i == 0 else rows[i - 1]
        for block, owner in ((mine[...], place + core), (other_ref[i], place + 1 - core)):
            depth = pl.ds(pl.multiple_of(owner * width, width), width)
            square += jnp.dot(block, cols_ref[depth, :], preferred_element_type=jnp.float32)
    row_index = band * height + lax.broadcasted_iota(jnp.int32, (height, width), 0)
    col_index = ga * width + lax.broadcasted_iota(jnp.int32, (height, width), 1)
    unit = (row_index == col_index).astype(jnp.float32)
    deviation = margin_ref[...] - unit
    fix_ref[...] = (unit - 0.5 * deviation + 0.375 * square).astype(fix_ref.dtype)


def final_kernel(groups, chips, orbitals_ref, *refs):
    parts = refs[: 2 * (groups - 1)]
    fix_own = refs[2 * (groups - 1)]
    fix_rows = refs[2 * groups - 1 : 2 * groups - 2 + chips]
    other_ref = refs[2 * groups - 2 + chips]
    out_ref, fix_ref = refs[-2:]
    band, ga = lax.axis_index("band"), lax.axis_index("ga")
    chip, core = ga // 2, lax.rem(ga, 2)
    width = fix_own.shape[1]
    for i in range(chips):
        mine = fix_own if i == 0 else fix_rows[i - 1]
        place = (chip ^ i) * 2
        fix_ref[place + core] = mine[...]
        fix_ref[place + 1 - core] = other_ref[i]
    half = parts[0].shape[0]
    spans = (pl.ds(0, half), pl.ds(half, orbitals_ref.shape[0] - half))
    share = 2 * chips // groups
    fixes = [
        jnp.concatenate([fix_ref[(band ^ r) * share + j] for j in range(share)], axis=1)
        for r in range(groups)
    ]
    for s, span in enumerate(spans):
        total = None
        for r in range(groups):
            if r == 0:
                piece = orbitals_ref[span, :]
            else:
                piece = parts[2 * r - 2 + s][...]
            term = lax.dot_general(
                piece, fixes[r], (((1,), (1,)), ((), ())), preferred_element_type=jnp.float32
            )
            total = term if total is None else total + term
        out_ref[span, :] = total.astype(out_ref.dtype)


def size_of(value):
    return value.size * value.dtype.itemsize


def call(kernel, outs, *args, scratch=(), flops=0):
    held = sum(size_of(leaf) for leaf in [*args, *jax.tree.leaves(outs)])
    return pl.pallas_call(
        kernel,
        out_shape=outs,
        in_specs=[VMEM] * len(args),
        out_specs=jax.tree.map(lambda _: VMEM, outs),
        scratch_shapes=list(scratch),
        cost_estimate=pl.CostEstimate(flops=flops, bytes_accessed=0, transcendentals=0),
        compiler_params=pltpu.CompilerParams(vmem_limit_bytes=min(2 * held + GRANT, 60 * GRANT // 4)),
    )(*args)


def far_first(chips):
    return [*range(2, chips), *range(1, min(2, chips))]


def gather_chips(block, chips, beside=0):
    order = far_first(chips)
    moves = [("ga", 2 * i) for i in order]
    moves += [("band", r) for r in range(beside, 0, -1)]
    landed = lax.optimization_barrier([swap(block, axis, mask) for axis, mask in moves])
    landed = dict(zip(moves, landed))
    rows = [landed["ga", 2 * i] for i in range(1, chips)]
    cols = [landed["band", r] for r in range(1, beside + 1)]
    other = swap(jnp.stack([block] + rows), "ga", 1)
    return rows, other, cols


def shards(orbitals):
    own_coeffs, own_bands = orbitals.shape
    groups, size = lax.axis_size("band"), lax.axis_size("ga")
    chips = size // 2
    all_bands = own_bands * groups
    all_coeffs = own_coeffs * size
    width = all_bands // size
    row_start = lax.axis_index("band") * own_bands
    col_start = lax.axis_index("ga") * width

    bands = gather_bands(orbitals)
    parts = [piece for pieces in bands[1:] for piece in pieces]
    keep, send = call(
        functools.partial(partial_kernel, groups, chips),
        (
            jax.ShapeDtypeStruct((chips, own_bands, width), jnp.float32),
            jax.ShapeDtypeStruct((chips, own_bands, width), jnp.bfloat16),
        ),
        orbitals,
        *parts,
        flops=2 * own_coeffs * own_bands * all_bands,
    )
    chip_sum = keep + swap(send, "ga", 1).astype(jnp.float32)
    total = chip_sum[0]
    for i in far_first(chips):
        total += swap(chip_sum[i].astype(jnp.bfloat16), "ga", 2 * i).astype(jnp.float32)
    margin_block = total / all_coeffs

    row_index = row_start + lax.iota(jnp.int32, own_bands)
    col_index = col_start + lax.iota(jnp.int32, width)
    unit_block = (row_index[:, None] == col_index[None, :]).astype(jnp.float32)
    deviation = (margin_block - unit_block).astype(jnp.bfloat16)
    rows, other, cols = gather_chips(deviation, chips, groups - 1)
    fix_block = call(
        functools.partial(fix_kernel, groups, chips),
        jax.ShapeDtypeStruct((own_bands, width), jnp.bfloat16),
        margin_block,
        deviation,
        *rows,
        other,
        *cols,
        scratch=[pltpu.VMEM((all_bands, width), jnp.bfloat16)],
        flops=2 * own_bands * all_bands * width,
    )
    fix_rows, fix_other, _ = gather_chips(fix_block, chips)
    corrected = call(
        functools.partial(final_kernel, groups, chips),
        jax.ShapeDtypeStruct(orbitals.shape, jnp.bfloat16),
        orbitals,
        *parts,
        fix_block,
        *fix_rows,
        fix_other,
        scratch=[pltpu.VMEM((size, own_bands, width), jnp.bfloat16)],
        flops=2 * own_coeffs * own_bands * all_bands,
    )
    return (margin_block, corrected)


def solution(mesh):
    return jax.shard_map(
        shards,
        mesh=mesh,
        in_specs=(P("ga", "band"),),
        out_specs=(P("band", "ga"), P("ga", "band")),
        check_vma=False,
    )
```

```python
import functools

import jax
import jax.numpy as jnp
from jax import lax
from jax.experimental import pallas as pl
from jax.experimental.pallas import tpu as pltpu
from jax.sharding import PartitionSpec as P

GRANT = 4 * 2**20
VMEM = pl.BlockSpec(memory_space=pltpu.VMEM)


def swap(value, axis, mask):
    size = lax.axis_size(axis)
    return lax.ppermute(value, axis, [(i, i ^ mask) for i in range(size)])


def gather_bands(orbitals):
    size = lax.axis_size("band")
    half = orbitals.shape[0] // 2
    pieces = [orbitals[:half], orbitals[half:]]
    if size != 4:
        everyone = lax.all_gather(orbitals, "band", axis=0)
        me = lax.axis_index("band")
        others = [
            lax.dynamic_index_in_dim(everyone, me ^ r, keepdims=False) for r in range(1, size)
        ]
        return [pieces] + [[o[:half], o[half:]] for o in others]
    top, low = pieces
    top1, low2 = swap(top, "band", 1), swap(low, "band", 2)
    low1, top2 = swap(low, "band", 1), swap(top, "band", 2)
    top3, low3 = swap(top1, "band", 2), swap(low2, "band", 1)
    return [pieces, [top1, low1], [top2, low2], [top3, low3]]


def partial_kernel(pairs, with_own, own_ref, *refs):
    parts, (keep_ref, send_ref) = refs[:-2], refs[-2:]
    is_first = lax.rem(lax.axis_index("ga"), 2) == 0
    width = keep_ref.shape[2]
    pieces = [parts[p : p + 2] for p in range(0, len(parts), 2)]
    if with_own:
        pieces = [(own_ref,)] + pieces
    for r, piece in enumerate(pieces):
        start, block = 0, None
        for ref in piece:
            stop = start + ref.shape[0]
            term = lax.dot_general(
                own_ref[start:stop, :], ref[...], (((0,), (0,)), ((), ())),
                preferred_element_type=jnp.float32,
            )
            start, block = stop, term if block is None else block + term
        for j in range(pairs):
            left = block[:, 2 * j * width : (2 * j + 1) * width]
            right = block[:, (2 * j + 1) * width : (2 * j + 2) * width]
            keep_ref[r * pairs + j] = jnp.where(is_first, left, right)
            send_ref[r * pairs + j] = jnp.where(is_first, right, left).astype(send_ref.dtype)


def fix_kernel(groups, chips, margin_ref, own_ref, *refs):
    rows, other_ref = refs[: chips - 1], refs[chips - 1]
    cols = refs[chips : chips + groups - 1]
    fix_ref, cols_ref = refs[-2:]
    band, ga = lax.axis_index("band"), lax.axis_index("ga")
    chip, core = ga // 2, lax.rem(ga, 2)
    height, width = margin_ref.shape
    for r in range(groups):
        source = own_ref if r == 0 else cols[r - 1]
        cols_ref[pl.ds(pl.multiple_of((band ^ r) * height, height), height), :] = source[...]
    square = jnp.zeros((height, width), jnp.float32)
    for i in range(chips):
        place = (chip ^ i) * 2
        mine = own_ref if i == 0 else rows[i - 1]
        for block, owner in ((mine[...], place + core), (other_ref[i], place + 1 - core)):
            depth = pl.ds(pl.multiple_of(owner * width, width), width)
            square += jnp.dot(block, cols_ref[depth, :], preferred_element_type=jnp.float32)
    row_index = band * height + lax.broadcasted_iota(jnp.int32, (height, width), 0)
    col_index = ga * width + lax.broadcasted_iota(jnp.int32, (height, width), 1)
    unit = (row_index == col_index).astype(jnp.float32)
    deviation = margin_ref[...] - unit
    fix_ref[...] = (unit - 0.5 * deviation + 0.375 * square).astype(fix_ref.dtype)


def final_kernel(groups, chips, orbitals_ref, *refs):
    parts = refs[: 2 * (groups - 1)]
    fix_own = refs[2 * (groups - 1)]
    fix_rows = refs[2 * groups - 1 : 2 * groups - 2 + chips]
    other_ref = refs[2 * groups - 2 + chips]
    out_ref, fix_ref = refs[-2:]
    band, ga = lax.axis_index("band"), lax.axis_index("ga")
    chip, core = ga // 2, lax.rem(ga, 2)
    width = fix_own.shape[1]
    for i in range(chips):
        mine = fix_own if i == 0 else fix_rows[i - 1]
        place = (chip ^ i) * 2
        fix_ref[place + core] = mine[...]
        fix_ref[place + 1 - core] = other_ref[i]
    half = orbitals_ref.shape[0] // 2
    share = 2 * chips // groups
    fixes = [
        jnp.concatenate([fix_ref[(band ^ r) * share + j] for j in range(share)], axis=1)
        for r in range(groups)
    ]
    for s in range(2):
        total = None
        for r in range(groups):
            if r == 0:
                piece = orbitals_ref[s * half : (s + 1) * half, :]
            else:
                piece = parts[2 * r - 2 + s][...]
            term = lax.dot_general(
                piece, fixes[r], (((1,), (1,)), ((), ())), preferred_element_type=jnp.float32
            )
            total = term if total is None else total + term
        out_ref[s * half : (s + 1) * half, :] = total.astype(out_ref.dtype)


def size_of(value):
    return value.size * value.dtype.itemsize


def call(kernel, outs, *args, scratch=(), flops=0):
    held = sum(size_of(leaf) for leaf in [*args, *jax.tree.leaves(outs)])
    return pl.pallas_call(
        kernel,
        out_shape=outs,
        in_specs=[VMEM] * len(args),
        out_specs=jax.tree.map(lambda _: VMEM, outs),
        scratch_shapes=list(scratch),
        cost_estimate=pl.CostEstimate(flops=flops, bytes_accessed=0, transcendentals=0),
        compiler_params=pltpu.CompilerParams(vmem_limit_bytes=min(2 * held + GRANT, 60 * GRANT // 4)),
    )(*args)


def far_first(chips):
    return [*range(2, chips), *range(1, min(2, chips))]


def gather_chips(block, chips, beside=0):
    order = far_first(chips)
    moves = [("ga", 2 * i) for i in order[:-1]]
    moves += [("band", r) for r in range(beside, 0, -1)]
    moves += [("ga", 2 * i) for i in order[-1:]]
    landed = lax.optimization_barrier([swap(block, axis, mask) for axis, mask in moves])
    landed = dict(zip(moves, landed))
    rows = [landed["ga", 2 * i] for i in range(1, chips)]
    cols = [landed["band", r] for r in range(1, beside + 1)]
    other = swap(jnp.stack([block] + rows), "ga", 1)
    return rows, other, cols


def shards(orbitals):
    own_coeffs, own_bands = orbitals.shape
    groups, size = lax.axis_size("band"), lax.axis_size("ga")
    chips = size // 2
    all_bands = own_bands * groups
    all_coeffs = own_coeffs * size
    width = all_bands // size
    row_start = lax.axis_index("band") * own_bands
    col_start = lax.axis_index("ga") * width

    bands = gather_bands(orbitals)
    parts = [piece for pieces in bands[1:] for piece in pieces]
    pairs = chips // groups
    sums = []
    for count, with_own, some in ((groups - 1, True, parts[:-2]), (1, False, parts[-2:])):
        keep, send = call(
            functools.partial(partial_kernel, pairs, with_own),
            tuple(
                jax.ShapeDtypeStruct((count * pairs, own_bands, width), dtype)
                for dtype in (jnp.float32, jnp.bfloat16)
            ),
            orbitals,
            *some,
            flops=2 * own_coeffs * own_bands * own_bands * count,
        )
        sums.append(keep + swap(send, "ga", 1).astype(jnp.float32))
    by_group = jnp.concatenate(sums)
    here = (lax.axis_index("ga") // 2) ^ (lax.axis_index("band") * pairs)
    chip_sum = [
        lax.dynamic_index_in_dim(by_group, here ^ i, keepdims=False) for i in range(chips)
    ]
    total = chip_sum[0]
    for i in far_first(chips):
        total += swap(chip_sum[i].astype(jnp.bfloat16), "ga", 2 * i).astype(jnp.float32)
    margin_block = total / all_coeffs

    row_index = row_start + lax.iota(jnp.int32, own_bands)
    col_index = col_start + lax.iota(jnp.int32, width)
    unit_block = (row_index[:, None] == col_index[None, :]).astype(jnp.float32)
    deviation = (margin_block - unit_block).astype(jnp.bfloat16)
    rows, other, cols = gather_chips(deviation, chips, groups - 1)
    fix_block = call(
        functools.partial(fix_kernel, groups, chips),
        jax.ShapeDtypeStruct((own_bands, width), jnp.bfloat16),
        margin_block,
        deviation,
        *rows,
        other,
        *cols,
        scratch=[pltpu.VMEM((all_bands, width), jnp.bfloat16)],
        flops=2 * own_bands * all_bands * width,
    )
    fix_rows, fix_other, _ = gather_chips(fix_block, chips)
    corrected = call(
        functools.partial(final_kernel, groups, chips),
        jax.ShapeDtypeStruct(orbitals.shape, jnp.bfloat16),
        orbitals,
        *parts,
        fix_block,
        *fix_rows,
        fix_other,
        scratch=[pltpu.VMEM((size, own_bands, width), jnp.bfloat16)],
        flops=2 * own_coeffs * own_bands * all_bands,
    )
    return (margin_block, corrected)


def solution(mesh):
    return jax.shard_map(
        shards,
        mesh=mesh,
        in_specs=(P("ga", "band"),),
        out_specs=(P("band", "ga"), P("ga", "band")),
        check_vma=False,
    )
```
